8 devices in a mesh: dp: 8 (over z, y, x, core).
Axes of the slice: x: 2, y: 2, z: 1, core: 2. Of those that a mesh axis runs over, the one named last changes fastest.
Arguments:
- local_grads: bfloat16 [8, 32768, 1024], P('dp')
- master: float32 [32768, 1024], P('dp')
- mom_first: float32 [32768, 1024], P('dp')
- mom_second: float32 [32768, 1024], P('dp')
- learn_rate: float32 [], replicated
Outputs:
- output 1: float32 [32768, 1024], P('dp')
- output 2: float32 [32768, 1024], P('dp')
- output 3: float32 [32768, 1024], P('dp')
- output 4: bfloat16 [32768, 1024], replicated
All inputs are finite; a program needn't handle non-finite values.
Results may differ from the reference program's by a relative error of at most 0.001.
Values are sent between devices in bfloat16 or wider.
A program may use at most 1 GiB of HBM per device.

```python
import math
import jax
import jax.numpy as jnp
import numpy as np
from jax import lax

D = 1024
ROWS_DEV = 4096
DEVICES = 8
LAYERS = 2
MIX_RANK = 32
DECAY_RANK = 64
ADAM_STEP = 10


def rule_table(model_width, total_rows):
    ffn_width = 7 * model_width // 2
    layer_rows = 6 * model_width + 2 * ffn_width + 16 + 10 * MIX_RANK + 2 * DECAY_RANK
    vocab_rows = (total_rows - LAYERS * layer_rows - 4) // 2
    base_rule = (1.0, 0.0)
    decay_rule = (1.0, 0.1)
    time_rule = (2.0, 0.0)
    pieces = [(vocab_rows, decay_rule)]
    for layer_idx in range(LAYERS):
        lead_rows = 12 if layer_idx == 0 else 10
        pieces = pieces + [(lead_rows + 10 * MIX_RANK, base_rule), (1, time_rule), (2 * DECAY_RANK, base_rule), (1, time_rule), (5 * model_width, decay_rule), (4, base_rule), (2 * ffn_width + model_width, decay_rule)]
    pieces = pieces + [(2, base_rule), (vocab_rows, decay_rule)]
    run_lengths = np.array([run_len for run_len, run_rule in pieces])
    lr_factor = np.repeat(np.array([run_rule[0] for run_len, run_rule in pieces]), run_lengths)
    decay_rate = np.repeat(np.array([run_rule[1] for run_len, run_rule in pieces]), run_lengths)
    return lr_factor, decay_rate


def setup_inputs(seed: int = 0) -> dict:
    key_grad, key_master, key_first, key_second, key_rate = jax.random.split(jax.random.key(seed), 5)
    total_rows = DEVICES * ROWS_DEV
    elem_count = total_rows * D
    grad_scale = 3.0 * math.sqrt(DEVICES / elem_count)
    clip_unit = 1.0 / math.sqrt(elem_count)

    def draw_device(dev_key):
        gauss_noise = jax.random.normal(dev_key, (total_rows, D), jnp.float32)
        return (grad_scale * gauss_noise).astype(jnp.bfloat16)

    local_grads = lax.map(draw_device, jax.random.split(key_grad, DEVICES))
    master = (0.5 / math.sqrt(D)) * jax.random.normal(key_master, (total_rows, D), jnp.float32)
    mom_first = 0.1 * clip_unit * jax.random.normal(key_first, (total_rows, D), jnp.float32)
    mom_second = jnp.square(0.1 * clip_unit * jax.random.uniform(key_second, (total_rows, D), jnp.float32, 0.5, 1.5))
    learn_rate = jax.random.uniform(key_rate, (), jnp.float32, 0.005, 0.015)
    return {'local_grads': local_grads, 'master': master, 'mom_first': mom_first, 'mom_second': mom_second, 'learn_rate': learn_rate}


def reference(local_grads, master, mom_first, mom_second, learn_rate):
    def add_device(running, grad_block):
        return running + grad_block.astype(jnp.float32), None

    grad_total = lax.scan(add_device, jnp.zeros(master.shape, jnp.float32), local_grads)[0]
    grad_mean = grad_total / local_grads.shape[0]
    grad_norm = jnp.sqrt(jnp.sum(grad_mean * grad_mean))
    clip_scale = jnp.minimum(1.0, 1.0 / (grad_norm + 1e-6))
    clipped = grad_mean * clip_scale
    new_first = 0.9 * mom_first + 0.1 * clipped
    new_second = 0.99 * mom_second + 0.01 * (clipped * clipped)
    first_hat = new_first / (1.0 - 0.9 ** ADAM_STEP)
    second_hat = new_second / (1.0 - 0.99 ** ADAM_STEP)
    lr_factor, decay_rate = rule_table(master.shape[1], master.shape[0])
    row_rate = learn_rate * jnp.asarray(lr_factor, jnp.float32)[:, None]
    row_decay = jnp.asarray(decay_rate, jnp.float32)[:, None]
    new_master = master - row_rate * (first_hat / (jnp.sqrt(second_hat) + 1e-8) + row_decay * master)
    return new_master, new_first, new_second, new_master.astype(jnp.bfloat16)
```

```python
import functools

import jax
import jax.numpy as jnp
from jax import lax
from jax.experimental import pallas as pl
from jax.experimental.pallas import tpu as pltpu
from jax.sharding import PartitionSpec as P

LAYERS = 2
MIX_RANK = 32
DECAY_RANK = 64
ADAM_STEP = 10

MESH = pl.DeviceIdType.MESH
CHUNK = 256
DIRECT = 1024
GROUP = 16
BLOCK = 256
PARTS = (512, 1536, 1536, 512)


def layout_runs(model_width, total_rows):
    ffn_width = 7 * model_width // 2
    layer_rows = 6 * model_width + 2 * ffn_width + 16 + 10 * MIX_RANK + 2 * DECAY_RANK
    vocab_rows = (total_rows - LAYERS * layer_rows - 4) // 2
    base_rule = (1.0, 0.0)
    decay_rule = (1.0, 0.1)
    time_rule = (2.0, 0.0)
    pieces = [(vocab_rows, decay_rule)]
    for layer_idx in range(LAYERS):
        lead_rows = 12 if layer_idx == 0 else 10
        pieces = pieces + [(lead_rows + 10 * MIX_RANK, base_rule), (1, time_rule), (2 * DECAY_RANK, base_rule), (1, time_rule), (5 * model_width, decay_rule), (4, base_rule), (2 * ffn_width + model_width, decay_rule)]
    pieces = pieces + [(2, base_rule), (vocab_rows, decay_rule)]
    runs = []
    next_row = 0
    for run_len, run_rule in pieces:
        runs.append((next_row, run_rule[0], run_rule[1]))
        next_row = next_row + run_len
    return runs


def reduce_kernel(half, grads, total, clip, rx, pd, p2, stage, own, other, near0, near1, last, result, squares, norms,
                  p1_send, direct_send, pair_send, p2_send, norm_send, rx_sem, direct_sem, pair_sem, p2_sem, norm_sem, load_sem, store_sem):
    me = lax.axis_index("dp")
    count = 8
    core = lax.rem(me, 2)
    chip = lax.div(me, 2)
    x, y = lax.rem(chip, 2), lax.div(chip, 2)
    x_near, y_near = y * 2 + 1 - x, (1 - y) * 2 + x
    diagonal = (1 - y) * 2 + 1 - x
    first = (x_near, y_near)
    second = (y_near, x_near)
    partner = chip * 2 + 1 - core
    chunks = half // CHUNK
    directs = half // DIRECT

    barrier = pltpu.get_barrier_semaphore()
    for step in range(1, count):
        pl.semaphore_signal(barrier, inc=1, device_id=(lax.rem(me + step, count),), device_id_type=MESH)
    pl.semaphore_wait(barrier, count - 1)

    def forward_copy(h, to_core, k):
        rows = pl.ds(h * half + k * CHUNK, CHUNK)
        return pltpu.make_async_remote_copy(
            src_ref=grads.at[diagonal * 2 + to_core, rows], dst_ref=rx.at[h, 0, core, pl.ds(k * CHUNK, CHUNK)],
            send_sem=p1_send.at[h, to_core, k], recv_sem=rx_sem.at[h, core, k],
            device_id=(first[h] * 2 + to_core,), device_id_type=MESH)

    def direct_copy(h, to_core, k):
        rows = pl.ds(h * half + k * DIRECT, DIRECT)
        return pltpu.make_async_remote_copy(
            src_ref=grads.at[first[h] * 2 + to_core, rows], dst_ref=rx.at[h, 1, core, pl.ds(k * DIRECT, DIRECT)],
            send_sem=direct_send.at[h, to_core, k], recv_sem=direct_sem.at[h, core, k],
            device_id=(first[h] * 2 + to_core,), device_id_type=MESH)

    def pair_copy(h, kind):
        owner = (second[h] if kind == 0 else chip) * 2 + 1 - core
        return pltpu.make_async_remote_copy(
            src_ref=grads.at[owner, pl.ds(h * half, half)], dst_ref=pd.at[h, kind],
            send_sem=pair_send.at[h, kind], recv_sem=pair_sem.at[h, kind],
            device_id=(partner,), device_id_type=MESH)

    def second_copy(h, k):
        rows = pl.ds(k * CHUNK, CHUNK)
        return pltpu.make_async_remote_copy(
            src_ref=stage.at[h, rows], dst_ref=p2.at[h, rows],
            send_sem=p2_send.at[h, k], recv_sem=p2_sem.at[h, k],
            device_id=(second[h] * 2 + core,), device_id_type=MESH)

    for k in range(chunks):
        for h in range(2):
            for to_core in range(2):
                forward_copy(h, to_core, k).start()
        if k == 0:
            for h in range(2):
                pair_copy(h, 0).start()
        if k == 2:
            for h in range(2):
                pair_copy(h, 1).start()
    for k in range(directs):
        for h in range(2):
            for to_core in range(2):
                direct_copy(h, to_core, k).start()

    def loads(h, kind, k):
        owner = (second[h] if kind == 0 else chip) * 2 + core
        rows = pl.ds(k * CHUNK, CHUNK)
        copies = [
            pltpu.make_async_copy(grads.at[owner, pl.ds(h * half + k * CHUNK, CHUNK)], own, load_sem.at[0]),
            pltpu.make_async_copy(pd.at[h, kind, rows], other, load_sem.at[1]),
            pltpu.make_async_copy(rx.at[h, kind, 0, rows], near0, load_sem.at[2]),
            pltpu.make_async_copy(rx.at[h, kind, 1, rows], near1, load_sem.at[3]),
        ]
        if kind == 1:
            copies.append(pltpu.make_async_copy(p2.at[h, rows], last, load_sem.at[4]))
        for copy in copies:
            copy.start()
        for copy in copies:
            copy.wait()

    def four(rows):
        return (own[rows].astype(jnp.float32) + other[rows].astype(jnp.float32)) + (near0[rows].astype(jnp.float32) + near1[rows].astype(jnp.float32))

    for h in range(2):
        pair_copy(h, 0).wait_recv()

    def forward_step(k, carry):
        for h in range(2):
            for from_core in range(2):
                pltpu.make_async_copy(rx.at[h, 0, from_core, pl.ds(0, CHUNK)], rx.at[h, 0, from_core, pl.ds(0, CHUNK)], rx_sem.at[h, from_core, k]).wait()
            loads(h, 0, k)

            def add(group, carry):
                base = pl.multiple_of(group * GROUP, GROUP)
                stage[h, pl.ds(pl.multiple_of(k * CHUNK + base, GROUP), GROUP)] = four(pl.ds(base, GROUP))
                return carry

            lax.fori_loop(0, CHUNK // GROUP, add, 0)
            second_copy(h, k).start()
        return carry

    lax.fori_loop(0, chunks, forward_step, 0)

    for h in range(2):
        pair_copy(h, 1).wait_recv()
        for from_core in range(2):
            for k in range(directs):
                rows = pl.ds(k * DIRECT, DIRECT)
                pltpu.make_async_copy(rx.at[h, 1, from_core, rows], rx.at[h, 1, from_core, rows], direct_sem.at[h, from_core, k]).wait()

    squares[...] = jnp.zeros_like(squares)

    def owner_step(k, carry):
        for h in range(2):
            second_copy(h, k).wait_recv()
            loads(h, 1, k)

            def add(group, carry):
                rows = pl.ds(pl.multiple_of(group * GROUP, GROUP), GROUP)
                mean = (four(rows) + last[rows]) * (1.0 / count)
                result[rows] = mean
                squares[...] += mean * mean
                return carry

            lax.fori_loop(0, CHUNK // GROUP, add, 0)
            store = pltpu.make_async_copy(result, total.at[pl.ds(h * half + k * CHUNK, CHUNK)], store_sem.at[0])
            store.start()
            store.wait()
        return carry

    lax.fori_loop(0, chunks, owner_step, 0)

    lanes = jnp.sum(squares[...].reshape(GROUP // 8, 8, squares.shape[1]), axis=0)
    partial = lanes[:, 0:128]
    for column in range(1, squares.shape[1] // 128):
        partial += lanes[:, column * 128:(column + 1) * 128]
    norms[me] = partial

    for h in range(2):
        for to_core in range(2):
            for k in range(chunks):
                forward_copy(h, to_core, k).wait_send()
            for k in range(directs):
                direct_copy(h, to_core, k).wait_send()
        for kind in range(2):
            pair_copy(h, kind).wait_send()
        for k in range(chunks):
            second_copy(h, k).wait_send()

    def norm_copy(step):
        to = lax.rem(me + step, count)
        return pltpu.make_async_remote_copy(
            src_ref=norms.at[me], dst_ref=norms.at[me], send_sem=norm_send.at[step], recv_sem=norm_sem.at[me],
            device_id=(to,), device_id_type=MESH)

    for step in range(1, count):
        norm_copy(step).start()
    for step in range(1, count):
        source = lax.rem(me + step, count)
        pltpu.make_async_copy(norms.at[source], norms.at[source], norm_sem.at[source]).wait()
    for step in range(1, count):
        norm_copy(step).wait_send()
    square_sum = jnp.sum(jnp.sum(norms[...], axis=0))
    norm = jnp.sqrt(jnp.full(clip.shape, square_sum, jnp.float32))
    clip[...] = jnp.minimum(1.0, 1.0 / (norm + 1e-6))


def reduce_gradients(local_grads, count):
    _, total_rows, width = local_grads.shape
    rows = total_rows // count
    half = rows // 2
    chunks, directs = half // CHUNK, half // DIRECT
    any_space = pl.BlockSpec(memory_space=pl.ANY)
    outs = pl.pallas_call(
        functools.partial(reduce_kernel, half),
        name="reduce_gradients",
        out_shape=(
            jax.ShapeDtypeStruct((rows, width), jnp.float32),
            jax.ShapeDtypeStruct((8, 128), jnp.float32),
            jax.ShapeDtypeStruct((2, 2, 2, half, width), jnp.bfloat16),
            jax.ShapeDtypeStruct((2, 2, half, width), jnp.bfloat16),
            jax.ShapeDtypeStruct((2, half, width), jnp.float32),
        ),
        in_specs=[any_space],
        out_specs=(any_space, pl.BlockSpec(memory_space=pltpu.VMEM), any_space, any_space, any_space),
        scratch_shapes=[
            pltpu.VMEM((2, half, width), jnp.float32),
            pltpu.VMEM((CHUNK, width), jnp.bfloat16),
            pltpu.VMEM((CHUNK, width), jnp.bfloat16),
            pltpu.VMEM((CHUNK, width), jnp.bfloat16),
            pltpu.VMEM((CHUNK, width), jnp.bfloat16),
            pltpu.VMEM((CHUNK, width), jnp.float32),
            pltpu.VMEM((CHUNK, width), jnp.float32),
            pltpu.VMEM((GROUP, width), jnp.float32),
            pltpu.VMEM((count, 8, 128), jnp.float32),
            pltpu.SemaphoreType.DMA((2, 2, chunks)),
            pltpu.SemaphoreType.DMA((2, 2, directs)),
            pltpu.SemaphoreType.DMA((2, 2)),
            pltpu.SemaphoreType.DMA((2, chunks)),
            pltpu.SemaphoreType.DMA((count,)),
            pltpu.SemaphoreType.DMA((2, 2, chunks)),
            pltpu.SemaphoreType.DMA((2, 2, directs)),
            pltpu.SemaphoreType.DMA((2, 2)),
            pltpu.SemaphoreType.DMA((2, chunks)),
            pltpu.SemaphoreType.DMA((count,)),
            pltpu.SemaphoreType.DMA((5,)),
            pltpu.SemaphoreType.DMA((1,)),
        ],
        compiler_params=pltpu.CompilerParams(collective_id=0, has_side_effects=True, vmem_limit_bytes=60 * 1024 * 1024),
    )(local_grads.reshape(count, rows, width))
    return outs[0], outs[1]


def update_kernel(start, shard_rows, runs, has_state, learn_rate, clip, grad, master, first, second, *refs):
    new_master, new_first, new_second, working = refs[3:7] if has_state else refs[0:4]
    block = grad.shape[0]
    base = lax.axis_index("dp") * shard_rows + start + pl.program_id(0) * block
    row = base + lax.broadcasted_iota(jnp.int32, (block, 128), 0)
    factor = jnp.full((block, 128), runs[0][1], jnp.float32)
    decay = jnp.full((block, 128), runs[0][2], jnp.float32)
    for before, run in zip(runs[:-1], runs[1:]):
        later = row >= run[0]
        if run[1] != before[1]:
            factor = jnp.where(later, run[1], factor)
        if run[2] != before[2]:
            decay = jnp.where(later, run[2], decay)
    step_size = learn_rate[0] * factor
    scale = clip[0:1, :]
    for column in range(grad.shape[1] // 128):
        lanes = pl.ds(column * 128, 128)
        clipped = grad[:, lanes] * scale
        first_value = 0.9 * first[:, lanes] + 0.1 * clipped
        second_value = 0.99 * second[:, lanes] + 0.01 * (clipped * clipped)
        first_hat = first_value * (1.0 / (1.0 - 0.9 ** ADAM_STEP))
        second_hat = second_value * (1.0 / (1.0 - 0.99 ** ADAM_STEP))
        old = master[:, lanes]
        value = old - step_size * (first_hat / (jnp.sqrt(second_hat) + 1e-8) + decay * old)
        new_master[:, lanes] = value
        new_first[:, lanes] = first_value
        new_second[:, lanes] = second_value
        working[:, lanes] = value.astype(jnp.bfloat16)


def update_rows(start, rows, runs, state, gathered_shape, learn_rate, clip, grad, master, first, second):
    shard_rows, width = grad.shape
    block = pl.BlockSpec((BLOCK, width), lambda i: (start // BLOCK + i, 0))
    any_space = pl.BlockSpec(memory_space=pl.ANY)
    in_specs = [pl.BlockSpec(memory_space=pltpu.SMEM), pl.BlockSpec((8, 128), lambda i: (0, 0)), block, block, block, block]
    args = [learn_rate, clip, grad, master, first, second]
    aliases = {}
    if state is not None:
        aliases = {len(args) + i: i for i in range(3)}
        in_specs += [any_space] * 3
        args += list(state)
    whole = jax.ShapeDtypeStruct((shard_rows, width), jnp.float32)
    out_shape = [whole, whole, whole, jax.ShapeDtypeStruct((rows, width), jnp.bfloat16)]
    out_specs = [block, block, block, pl.BlockSpec((BLOCK, width), lambda i: (i, 0))]
    if gathered_shape is not None:
        out_shape.append(gathered_shape)
        out_specs.append(any_space)
    size = rows * width
    return pl.pallas_call(
        functools.partial(update_kernel, start, shard_rows, runs, state is not None),
        name="update_rows",
        grid=(rows // BLOCK,),
        out_shape=tuple(out_shape),
        in_specs=in_specs,
        out_specs=tuple(out_specs),
        input_output_aliases=aliases,
        cost_estimate=pl.CostEstimate(flops=20 * size, bytes_accessed=30 * size, transcendentals=2 * size),
        compiler_params=pltpu.CompilerParams(dimension_semantics=("arbitrary",), vmem_limit_bytes=48 * 1024 * 1024),
    )(*args)


def place_kernel(gathered, working_in, working):
    working[...] = gathered[0]


def place_rows(start, working, gathered):
    count, rows, width = gathered.shape
    shard_rows = working.shape[0] // count
    size = rows * width * count
    return pl.pallas_call(
        place_kernel,
        name="place_rows",
        grid=(count, rows // 512),
        out_shape=jax.ShapeDtypeStruct(working.shape, working.dtype),
        in_specs=[pl.BlockSpec((1, 512, width), lambda d, i: (d, i, 0)), pl.BlockSpec(memory_space=pl.ANY)],
        out_specs=pl.BlockSpec((512, width), lambda d, i: (d * (shard_rows // 512) + start // 512 + i, 0)),
        input_output_aliases={1: 0},
        cost_estimate=pl.CostEstimate(flops=size, bytes_accessed=4 * size, transcendentals=0),
        compiler_params=pltpu.CompilerParams(dimension_semantics=("arbitrary", "arbitrary")),
    )(gathered, working)


def solution(mesh):
    count = mesh.shape["dp"]

    def device_step(local_grads, master, mom_first, mom_second, learn_rate):
        shard_rows, width = master.shape
        total_rows = shard_rows * count
        runs = layout_runs(width, total_rows)
        grad, clip = reduce_gradients(local_grads, count)
        rate = learn_rate.reshape(1)
        state = None
        start = 0
        gathered = []
        for index, rows in enumerate(PARTS):
            shape = jax.ShapeDtypeStruct((total_rows, width), jnp.bfloat16) if index == len(PARTS) - 1 else None
            outs = update_rows(start, rows, runs, state, shape, rate, clip, grad, master, mom_first, mom_second)
            state = outs[0:3]
            gathered.append((start, lax.all_gather(outs[3], "dp", axis=0, tiled=False)))
            start += rows
        working = outs[4]
        for start, block in gathered:
            working = place_rows(start, working, block)
        return state[0], state[1], state[2], working

    return jax.shard_map(device_step, mesh=mesh, in_specs=(P("dp", None, None), P("dp", None), P("dp", None), P("dp", None), P()), out_specs=(P("dp", None), P("dp", None), P("dp", None), P(None, None)), check_vma=False)
```

```python
import functools

import jax
import jax.numpy as jnp
from jax import lax
from jax.experimental import pallas as pl
from jax.experimental.pallas import tpu as pltpu
from jax.sharding import PartitionSpec as P

LAYERS = 2
MIX_RANK = 32
DECAY_RANK = 64
ADAM_STEP = 10

MESH = pl.DeviceIdType.MESH
CHUNK = 256
DIRECT = 1024
GROUP = 16
BLOCK = 256
PARTS = (512, 3072, 512)
PIECE = 512
DEPTH = 16


def layout_runs(model_width, total_rows):
    ffn_width = 7 * model_width // 2
    layer_rows = 6 * model_width + 2 * ffn_width + 16 + 10 * MIX_RANK + 2 * DECAY_RANK
    vocab_rows = (total_rows - LAYERS * layer_rows - 4) // 2
    base_rule = (1.0, 0.0)
    decay_rule = (1.0, 0.1)
    time_rule = (2.0, 0.0)
    pieces = [(vocab_rows, decay_rule)]
    for layer_idx in range(LAYERS):
        lead_rows = 12 if layer_idx == 0 else 10
        pieces = pieces + [(lead_rows + 10 * MIX_RANK, base_rule), (1, time_rule), (2 * DECAY_RANK, base_rule), (1, time_rule), (5 * model_width, decay_rule), (4, base_rule), (2 * ffn_width + model_width, decay_rule)]
    pieces = pieces + [(2, base_rule), (vocab_rows, decay_rule)]
    runs = []
    next_row = 0
    for run_len, run_rule in pieces:
        runs.append((next_row, run_rule[0], run_rule[1]))
        next_row = next_row + run_len
    return runs


def places(axis):
    me = lax.axis_index(axis)
    core, chip = lax.rem(me, 2), lax.div(me, 2)
    x, y = lax.rem(chip, 2), lax.div(chip, 2)
    return me, core, chip, y * 2 + 1 - x, (1 - y) * 2 + x, (1 - y) * 2 + 1 - x


def reduce_kernel(half, grads, total, clip, rx, pd, stage, inbox, mine, own, other, near0, near1, squares, norms,
                  p1_send, direct_send, pair_send, p2_send, norm_send, rx_sem, direct_sem, pair_sem, p2_sem, norm_sem, load_sem, store_sem):
    me, core, chip, x_near, y_near, diagonal = places("dp")
    count = 8
    first = (x_near, y_near)
    second = (y_near, x_near)
    partner = chip * 2 + 1 - core
    chunks = half // CHUNK
    directs = half // DIRECT

    barrier = pltpu.get_barrier_semaphore()
    for step in range(1, count):
        pl.semaphore_signal(barrier, inc=1, device_id=(lax.rem(me + step, count),), device_id_type=MESH)
    pl.semaphore_wait(barrier, count - 1)

    def forward_copy(h, to_core, k):
        rows = pl.ds(h * half + k * CHUNK, CHUNK)
        return pltpu.make_async_remote_copy(
            src_ref=grads.at[diagonal * 2 + to_core, rows], dst_ref=rx.at[h, 0, core, pl.ds(k * CHUNK, CHUNK)],
            send_sem=p1_send.at[h, to_core, k], recv_sem=rx_sem.at[h, core, k],
            device_id=(first[h] * 2 + to_core,), device_id_type=MESH)

    def direct_copy(h, to_core, k):
        rows = pl.ds(h * half + k * DIRECT, DIRECT)
        return pltpu.make_async_remote_copy(
            src_ref=grads.at[first[h] * 2 + to_core, rows], dst_ref=rx.at[h, 1, core, pl.ds(k * DIRECT, DIRECT)],
            send_sem=direct_send.at[h, to_core, k], recv_sem=direct_sem.at[h, core, k],
            device_id=(first[h] * 2 + to_core,), device_id_type=MESH)

    def pair_copy(h, kind):
        owner = (second[h] if kind == 0 else chip) * 2 + 1 - core
        return pltpu.make_async_remote_copy(
            src_ref=grads.at[owner, pl.ds(h * half, half)], dst_ref=pd.at[h, kind],
            send_sem=pair_send.at[h, kind], recv_sem=pair_sem.at[h, kind],
            device_id=(partner,), device_id_type=MESH)

    def second_copy(h, k):
        rows = pl.ds(k * CHUNK, CHUNK)
        return pltpu.make_async_remote_copy(
            src_ref=stage.at[h, rows], dst_ref=inbox.at[h, rows],
            send_sem=p2_send.at[h, k], recv_sem=p2_sem.at[h, k],
            device_id=(second[h] * 2 + core,), device_id_type=MESH)

    for k in range(chunks):
        for h in range(2):
            for to_core in range(2):
                forward_copy(h, to_core, k).start()
        if k == 0:
            for h in range(2):
                pair_copy(h, 0).start()
        if k == 2:
            for h in range(2):
                pair_copy(h, 1).start()
    for k in range(directs):
        for h in range(2):
            for to_core in range(2):
                direct_copy(h, to_core, k).start()

    def loads(h, kind, k):
        owner = (second[h] if kind == 0 else chip) * 2 + core
        rows = pl.ds(k * CHUNK, CHUNK)
        copies = [
            pltpu.make_async_copy(grads.at[owner, pl.ds(h * half + k * CHUNK, CHUNK)], own, load_sem.at[0]),
            pltpu.make_async_copy(pd.at[h, kind, rows], other, load_sem.at[1]),
            pltpu.make_async_copy(rx.at[h, kind, 0, rows], near0, load_sem.at[2]),
            pltpu.make_async_copy(rx.at[h, kind, 1, rows], near1, load_sem.at[3]),
        ]
        for copy in copies:
            copy.start()
        for copy in copies:
            copy.wait()

    def four(rows):
        return (own[rows].astype(jnp.float32) + other[rows].astype(jnp.float32)) + (near0[rows].astype(jnp.float32) + near1[rows].astype(jnp.float32))

    for h in range(2):
        pair_copy(h, 0).wait_recv()

    def forward_step(k, carry):
        for h in range(2):
            for from_core in range(2):
                pltpu.make_async_copy(rx.at[h, 0, from_core, pl.ds(0, CHUNK)], rx.at[h, 0, from_core, pl.ds(0, CHUNK)], rx_sem.at[h, from_core, k]).wait()
            loads(h, 0, k)

            def add(group, carry):
                base = pl.multiple_of(group * GROUP, GROUP)
                stage[h, pl.ds(pl.multiple_of(k * CHUNK + base, GROUP), GROUP)] = four(pl.ds(base, GROUP))
                return carry

            lax.fori_loop(0, CHUNK // GROUP, add, 0)
            second_copy(h, k).start()
        return carry

    lax.fori_loop(0, chunks, forward_step, 0)

    for h in range(2):
        pair_copy(h, 1).wait_recv()

    def own_step(k, carry):
        for h in range(2):
            loads(h, 1, k)

            def add(group, carry):
                base = pl.multiple_of(group * GROUP, GROUP)
                mine[h, pl.ds(pl.multiple_of(k * CHUNK + base, GROUP), GROUP)] = four(pl.ds(base, GROUP))
                return carry

            lax.fori_loop(0, CHUNK // GROUP, add, 0)
        return carry

    for part in range(directs):
        for h in range(2):
            for from_core in range(2):
                rows = pl.ds(part * DIRECT, DIRECT)
                pltpu.make_async_copy(rx.at[h, 1, from_core, rows], rx.at[h, 1, from_core, rows], direct_sem.at[h, from_core, part]).wait()
        lax.fori_loop(part * DIRECT // CHUNK, (part + 1) * DIRECT // CHUNK, own_step, 0)

    squares[...] = jnp.zeros_like(squares)

    def store(h, k):
        rows = pl.ds(k * CHUNK, CHUNK)
        return pltpu.make_async_copy(mine.at[h, rows], total.at[pl.ds(h * half + k * CHUNK, CHUNK)], store_sem.at[h, k])

    def owner_step(k, carry):
        for h in range(2):
            second_copy(h, k).wait_recv()

            def add(group, carry):
                rows = pl.ds(pl.multiple_of(k * CHUNK + group * GROUP, GROUP), GROUP)
                mean = (mine[h, rows] + inbox[h, rows]) * (1.0 / count)
                mine[h, rows] = mean
                squares[...] += mean * mean
                return carry

            lax.fori_loop(0, CHUNK // GROUP, add, 0)
            store(h, k).start()
        return carry

    lax.fori_loop(0, chunks, owner_step, 0)

    lanes = jnp.sum(squares[...].reshape(GROUP // 8, 8, squares.shape[1]), axis=0)
    partial = lanes[:, 0:128]
    for column in range(1, squares.shape[1] // 128):
        partial += lanes[:, column * 128:(column + 1) * 128]
    norms[me] = partial

    for h in range(2):
        for to_core in range(2):
            for k in range(chunks):
                forward_copy(h, to_core, k).wait_send()
            for k in range(directs):
                direct_copy(h, to_core, k).wait_send()
        for kind in range(2):
            pair_copy(h, kind).wait_send()
        for k in range(chunks):
            second_copy(h, k).wait_send()

    def norm_copy(step):
        to = lax.rem(me + step, count)
        return pltpu.make_async_remote_copy(
            src_ref=norms.at[me], dst_ref=norms.at[me], send_sem=norm_send.at[step], recv_sem=norm_sem.at[me],
            device_id=(to,), device_id_type=MESH)

    for step in range(1, count):
        norm_copy(step).start()
    for step in range(1, count):
        source = lax.rem(me + step, count)
        pltpu.make_async_copy(norms.at[source], norms.at[source], norm_sem.at[source]).wait()
    for step in range(1, count):
        norm_copy(step).wait_send()
    for h in range(2):
        for k in range(chunks):
            store(h, k).wait()
    square_sum = jnp.sum(jnp.sum(norms[...], axis=0))
    norm = jnp.sqrt(jnp.full(clip.shape, square_sum, jnp.float32))
    clip[...] = jnp.minimum(1.0, 1.0 / (norm + 1e-6))


def reduce_gradients(local_grads, count):
    _, total_rows, width = local_grads.shape
    rows = total_rows // count
    half = rows // 2
    chunks, directs = half // CHUNK, half // DIRECT
    any_space = pl.BlockSpec(memory_space=pl.ANY)
    outs = pl.pallas_call(
        functools.partial(reduce_kernel, half),
        name="reduce_gradients",
        out_shape=(
            jax.ShapeDtypeStruct((rows, width), jnp.float32),
            jax.ShapeDtypeStruct((8, 128), jnp.float32),
            jax.ShapeDtypeStruct((2, 2, 2, half, width), jnp.bfloat16),
            jax.ShapeDtypeStruct((2, 2, half, width), jnp.bfloat16),
        ),
        in_specs=[any_space],
        out_specs=(any_space, pl.BlockSpec(memory_space=pltpu.VMEM), any_space, any_space),
        scratch_shapes=[
            pltpu.VMEM((2, half, width), jnp.float32),
            pltpu.VMEM((2, half, width), jnp.float32),
            pltpu.VMEM((2, half, width), jnp.float32),
            pltpu.VMEM((CHUNK, width), jnp.bfloat16),
            pltpu.VMEM((CHUNK, width), jnp.bfloat16),
            pltpu.VMEM((CHUNK, width), jnp.bfloat16),
            pltpu.VMEM((CHUNK, width), jnp.bfloat16),
            pltpu.VMEM((GROUP, width), jnp.float32),
            pltpu.VMEM((count, 8, 128), jnp.float32),
            pltpu.SemaphoreType.DMA((2, 2, chunks)),
            pltpu.SemaphoreType.DMA((2, 2, directs)),
            pltpu.SemaphoreType.DMA((2, 2)),
            pltpu.SemaphoreType.DMA((2, chunks)),
            pltpu.SemaphoreType.DMA((count,)),
            pltpu.SemaphoreType.DMA((2, 2, chunks)),
            pltpu.SemaphoreType.DMA((2, 2, directs)),
            pltpu.SemaphoreType.DMA((2, 2)),
            pltpu.SemaphoreType.DMA((2, chunks)),
            pltpu.SemaphoreType.DMA((count,)),
            pltpu.SemaphoreType.DMA((4,)),
            pltpu.SemaphoreType.DMA((2, chunks)),
        ],
        compiler_params=pltpu.CompilerParams(collective_id=0, has_side_effects=True, vmem_limit_bytes=60 * 1024 * 1024),
    )(local_grads.reshape(count, rows, width))
    return outs[0], outs[1]


def update_kernel(start, shard_rows, runs, has_state, learn_rate, clip, grad, master, first, second, *refs):
    new_master, new_first, new_second, working = refs[3:7] if has_state else refs[0:4]
    block = grad.shape[0]
    base = lax.axis_index("dp") * shard_rows + start + pl.program_id(0) * block
    row = base + lax.broadcasted_iota(jnp.int32, (block, 128), 0)
    factor = jnp.full((block, 128), runs[0][1], jnp.float32)
    decay = jnp.full((block, 128), runs[0][2], jnp.float32)
    for before, run in zip(runs[:-1], runs[1:]):
        later = row >= run[0]
        if run[1] != before[1]:
            factor = jnp.where(later, run[1], factor)
        if run[2] != before[2]:
            decay = jnp.where(later, run[2], decay)
    step_size = learn_rate[0] * factor
    scale = clip[0:1, :]
    for column in range(grad.shape[1] // 128):
        lanes = pl.ds(column * 128, 128)
        clipped = grad[:, lanes] * scale
        first_value = 0.9 * first[:, lanes] + 0.1 * clipped
        second_value = 0.99 * second[:, lanes] + 0.01 * (clipped * clipped)
        first_hat = first_value * (1.0 / (1.0 - 0.9 ** ADAM_STEP))
        second_hat = second_value * (1.0 / (1.0 - 0.99 ** ADAM_STEP))
        old = master[:, lanes]
        value = old - step_size * (first_hat / (jnp.sqrt(second_hat) + 1e-8) + decay * old)
        new_master[:, lanes] = value
        new_first[:, lanes] = first_value
        new_second[:, lanes] = second_value
        working[:, lanes] = value.astype(jnp.bfloat16)


def update_rows(start, rows, runs, state, gathered_shape, learn_rate, clip, grad, master, first, second):
    shard_rows, width = grad.shape
    block = pl.BlockSpec((BLOCK, width), lambda i: (start // BLOCK + i, 0))
    any_space = pl.BlockSpec(memory_space=pl.ANY)
    in_specs = [pl.BlockSpec(memory_space=pltpu.SMEM), pl.BlockSpec((8, 128), lambda i: (0, 0)), block, block, block, block]
    args = [learn_rate, clip, grad, master, first, second]
    aliases = {}
    if state is not None:
        aliases = {len(args) + i: i for i in range(3)}
        in_specs += [any_space] * 3
        args += list(state)
    whole = jax.ShapeDtypeStruct((shard_rows, width), jnp.float32)
    out_shape = [whole, whole, whole, jax.ShapeDtypeStruct((rows, width), jnp.bfloat16)]
    out_specs = [block, block, block, pl.BlockSpec((BLOCK, width), lambda i: (i, 0))]
    if gathered_shape is not None:
        out_shape.append(gathered_shape)
        out_specs.append(any_space)
    size = rows * width
    return pl.pallas_call(
        functools.partial(update_kernel, start, shard_rows, runs, state is not None),
        name="update_rows",
        grid=(rows // BLOCK,),
        out_shape=tuple(out_shape),
        in_specs=in_specs,
        out_specs=tuple(out_specs),
        input_output_aliases=aliases,
        cost_estimate=pl.CostEstimate(flops=20 * size, bytes_accessed=30 * size, transcendentals=2 * size),
        compiler_params=pltpu.CompilerParams(dimension_semantics=("arbitrary",), vmem_limit_bytes=48 * 1024 * 1024),
    )(*args)


def gather_kernel(rows, source, later_in, gathered, later, own, near_send, far_send, pair_send, near_sem, far_sem, pair_sem, load_sem, store_sem):
    me, core, chip, x_near, y_near, diagonal = places("dp")
    partner = chip * 2 + 1 - core
    near = (x_near * 2 + core, y_near * 2 + core)
    far = diagonal * 2 + core
    half = rows // 2
    steps = half // CHUNK

    barrier = pltpu.get_barrier_semaphore()
    for device in (partner, near[0], near[1]):
        pl.semaphore_signal(barrier, inc=1, device_id=(device,), device_id_type=MESH)
    pl.semaphore_wait(barrier, 3)

    def span(h, k):
        return pl.ds(h * half + k * CHUNK, CHUNK)

    def near_copy(axis, h, k):
        return pltpu.make_async_remote_copy(
            src_ref=source.at[span(h, k)], dst_ref=gathered.at[me, span(h, k)],
            send_sem=near_send.at[axis, h, k], recv_sem=near_sem.at[axis, h, k],
            device_id=(near[axis],), device_id_type=MESH)

    def far_copy(h, k):
        return pltpu.make_async_remote_copy(
            src_ref=gathered.at[near[h], span(h, k)], dst_ref=gathered.at[near[h], span(h, k)],
            send_sem=far_send.at[h, k], recv_sem=far_sem.at[h, k],
            device_id=(near[1 - h],), device_id_type=MESH)

    def pair_copy(kind, h, k):
        if kind == 0:
            src, slab = source.at[span(h, k)], me
        else:
            slab = (near[0], near[1], far)[kind - 1]
            src = gathered.at[slab, span(h, k)]
        return pltpu.make_async_remote_copy(
            src_ref=src, dst_ref=gathered.at[slab, span(h, k)],
            send_sem=pair_send.at[kind, h, k], recv_sem=pair_sem.at[kind, h, k],
            device_id=(partner,), device_id_type=MESH)

    def arrived(slab, h, k, sem):
        pltpu.make_async_copy(gathered.at[slab, span(h, k)], gathered.at[slab, span(h, k)], sem).wait()

    for order in range(2):
        for k in range(steps):
            for axis in range(2):
                near_copy(axis, axis if order == 0 else 1 - axis, k).start()
    load = pltpu.make_async_copy(source, own, load_sem.at[0])
    load.start()

    def first_step(k, carry):
        for h in range(2):
            pair_copy(0, h, k).start()
        for h in range(2):
            arrived(near[h], h, k, near_sem.at[h, h, k])
            far_copy(h, k).start()
            pair_copy(1 + h, h, k).start()
        return carry

    lax.fori_loop(0, steps, first_step, 0)
    load.wait()
    store = pltpu.make_async_copy(own, gathered.at[me], store_sem.at[0])
    store.start()

    def second_step(k, carry):
        for axis in range(2):
            arrived(near[axis], 1 - axis, k, near_sem.at[axis, 1 - axis, k])
            pair_copy(1 + axis, 1 - axis, k).start()
        return carry

    lax.fori_loop(0, steps, second_step, 0)

    def third_step(k, carry):
        for h in range(2):
            arrived(far, h, k, far_sem.at[h, k])
            pair_copy(3, h, k).start()
        return carry

    lax.fori_loop(0, steps, third_step, 0)
    store.wait()

    def finish(k, carry):
        for h in range(2):
            for axis in range(2):
                near_copy(axis, h, k).wait_send()
            far_copy(h, k).wait_send()
            for kind in range(4):
                pair_copy(kind, h, k).wait_send()
            twin = (partner, x_near * 2 + 1 - core, y_near * 2 + 1 - core, diagonal * 2 + 1 - core)
            for kind in range(4):
                arrived(twin[kind], h, k, pair_sem.at[kind, h, k])
        return carry

    lax.fori_loop(0, steps, finish, 0)


def gather_rows(block, later, count):
    rows, width = block.shape
    steps = rows // 2 // CHUNK
    any_space = pl.BlockSpec(memory_space=pl.ANY)
    return pl.pallas_call(
        functools.partial(gather_kernel, rows),
        name="gather_rows",
        out_shape=(jax.ShapeDtypeStruct((count, rows, width), block.dtype), jax.ShapeDtypeStruct(later.shape, later.dtype)),
        in_specs=[any_space, any_space],
        out_specs=(any_space, any_space),
        input_output_aliases={1: 1},
        scratch_shapes=[
            pltpu.VMEM((rows, width), block.dtype),
            pltpu.SemaphoreType.DMA((2, 2, steps)),
            pltpu.SemaphoreType.DMA((2, steps)),
            pltpu.SemaphoreType.DMA((4, 2, steps)),
            pltpu.SemaphoreType.DMA((2, 2, steps)),
            pltpu.SemaphoreType.DMA((2, steps)),
            pltpu.SemaphoreType.DMA((4, 2, steps)),
            pltpu.SemaphoreType.DMA((1,)),
            pltpu.SemaphoreType.DMA((1,)),
        ],
        cost_estimate=pl.CostEstimate(flops=40 * rows * width * count, bytes_accessed=4 * rows * width * count, transcendentals=0),
        compiler_params=pltpu.CompilerParams(collective_id=1, has_side_effects=True, vmem_limit_bytes=60 * 1024 * 1024),
    )(block, later)


def place_kernel(start, gathered, working_in, working, ring, in_sem, out_sem):
    count, rows, _ = gathered.shape
    shard_rows = working.shape[0] // count
    pieces = [(device, row) for row in range(0, rows, PIECE) for device in range(count)]

    def read(i):
        device, row = pieces[i]
        return pltpu.make_async_copy(gathered.at[device, pl.ds(row, PIECE)], ring.at[i % DEPTH], in_sem.at[i % DEPTH])

    def write(i):
        device, row = pieces[i]
        return pltpu.make_async_copy(ring.at[i % DEPTH], working.at[pl.ds(device * shard_rows + start + row, PIECE)], out_sem.at[i % DEPTH])

    lead = DEPTH // 2
    for i in range(len(pieces) + lead):
        if i < len(pieces):
            if i >= DEPTH:
                write(i - DEPTH).wait()
            read(i).start()
        if i >= lead:
            read(i - lead).wait()
            write(i - lead).start()
    for i in range(max(0, len(pieces) - DEPTH), len(pieces)):
        write(i).wait()


def place_rows(start, working, gathered):
    count, rows, width = gathered.shape
    size = rows * width * count
    any_space = pl.BlockSpec(memory_space=pl.ANY)
    return pl.pallas_call(
        functools.partial(place_kernel, start),
        name="place_rows",
        out_shape=jax.ShapeDtypeStruct(working.shape, working.dtype),
        in_specs=[any_space, any_space],
        out_specs=any_space,
        input_output_aliases={1: 0},
        scratch_shapes=[
            pltpu.VMEM((DEPTH, PIECE, width), working.dtype),
            pltpu.SemaphoreType.DMA((DEPTH,)),
            pltpu.SemaphoreType.DMA((DEPTH,)),
        ],
        cost_estimate=pl.CostEstimate(flops=size, bytes_accessed=4 * size, transcendentals=0),
        compiler_params=pltpu.CompilerParams(vmem_limit_bytes=48 * 1024 * 1024),
    )(gathered, working)


def solution(mesh):
    count = mesh.shape["dp"]

    def device_step(local_grads, master, mom_first, mom_second, learn_rate):
        shard_rows, width = master.shape
        total_rows = shard_rows * count
        runs = layout_runs(width, total_rows)
        grad, clip = reduce_gradients(local_grads, count)
        rate = learn_rate.reshape(1)
        state = None
        start = 0
        blocks = []
        for index, rows in enumerate(PARTS):
            shape = jax.ShapeDtypeStruct((total_rows, width), jnp.bfloat16) if index == len(PARTS) - 1 else None
            outs = update_rows(start, rows, runs, state, shape, rate, clip, grad, master, mom_first, mom_second)
            state = outs[0:3]
            blocks.append(outs[3])
            start += rows
        working = outs[4]
        early = lax.all_gather(blocks[0], "dp", axis=0, tiled=False)
        middle, block = gather_rows(blocks[1], blocks[2], count)
        late = lax.all_gather(block, "dp", axis=0, tiled=False)
        working = place_rows(PARTS[0], working, middle)
        working = place_rows(0, working, early)
        working = place_rows(PARTS[0] + PARTS[1], working, late)
        return state[0], state[1], state[2], working

    return jax.shard_map(device_step, mesh=mesh, in_specs=(P("dp", None, None), P("dp", None), P("dp", None), P("dp", None), P()), out_specs=(P("dp", None), P("dp", None), P("dp", None), P(None, None)), check_vma=False)
```

```python
import functools

import jax
import jax.numpy as jnp
from jax import lax
from jax.experimental import pallas as pl
from jax.experimental.pallas import tpu as pltpu
from jax.sharding import PartitionSpec as P

LAYERS = 2
MIX_RANK = 32
DECAY_RANK = 64
ADAM_STEP = 10

MESH = pl.DeviceIdType.MESH
CHUNK = 256
DIRECT = 1024
GROUP = 16
TILE = 32
BLOCK = 256
LATE = 1024
PIECE = 512
DEPTH = 16


def layout_runs(model_width, total_rows):
    ffn_width = 7 * model_width // 2
    layer_rows = 6 * model_width + 2 * ffn_width + 16 + 10 * MIX_RANK + 2 * DECAY_RANK
    vocab_rows = (total_rows - LAYERS * layer_rows - 4) // 2
    base_rule = (1.0, 0.0)
    decay_rule = (1.0, 0.1)
    time_rule = (2.0, 0.0)
    pieces = [(vocab_rows, decay_rule)]
    for layer_idx in range(LAYERS):
        lead_rows = 12 if layer_idx == 0 else 10
        pieces = pieces + [(lead_rows + 10 * MIX_RANK, base_rule), (1, time_rule), (2 * DECAY_RANK, base_rule), (1, time_rule), (5 * model_width, decay_rule), (4, base_rule), (2 * ffn_width + model_width, decay_rule)]
    pieces = pieces + [(2, base_rule), (vocab_rows, decay_rule)]
    runs = []
    next_row = 0
    for run_len, run_rule in pieces:
        runs.append((next_row, run_rule[0], run_rule[1]))
        next_row = next_row + run_len
    return runs


def places(axis):
    me = lax.axis_index(axis)
    core, chip = lax.rem(me, 2), lax.div(me, 2)
    x, y = lax.rem(chip, 2), lax.div(chip, 2)
    return me, core, chip, y * 2 + 1 - x, (1 - y) * 2 + x, (1 - y) * 2 + 1 - x


def row_rules(base, rows, runs):
    row = base + lax.broadcasted_iota(jnp.int32, (rows, 128), 0)
    factor = jnp.full((rows, 128), runs[0][1], jnp.float32)
    decay = jnp.full((rows, 128), runs[0][2], jnp.float32)
    for before, run in zip(runs[:-1], runs[1:]):
        later = row >= run[0]
        if run[1] != before[1]:
            factor = jnp.where(later, run[1], factor)
        if run[2] != before[2]:
            decay = jnp.where(later, run[2], decay)
    return factor, decay


def adam(grad, scale, old, first, second, step_size, decay):
    clipped = grad * scale
    first_value = 0.9 * first + 0.1 * clipped
    second_value = 0.99 * second + 0.01 * (clipped * clipped)
    first_hat = first_value * (1.0 / (1.0 - 0.9 ** ADAM_STEP))
    second_hat = second_value * (1.0 / (1.0 - 0.99 ** ADAM_STEP))
    value = old - step_size * (first_hat / (jnp.sqrt(second_hat) + 1e-8) + decay * old)
    return value, first_value, second_value


def step_kernel(half, runs, learn_rate, grads, master, mom_first, mom_second, total, clip, rx, pd, stage, gathered, late,
                inbox, mine, own, other, near0, near1, tile, squares, norms, state, work,
                p1_send, direct_send, pair_send, p2_send, norm_send, rx_sem, direct_sem, pair_sem, p2_sem, norm_sem, load_sem, store_sem, stage_sem,
                state_sem, copy_sem, near_send, far_send, twin_send, near_sem, far_sem, twin_sem):
    me, core, chip, x_near, y_near, diagonal = places("dp")
    count = 8
    first = (x_near, y_near)
    second = (y_near, x_near)
    partner = chip * 2 + 1 - core
    chunks = half // CHUNK
    directs = half // DIRECT

    barrier = pltpu.get_barrier_semaphore()
    for step in range(1, count):
        pl.semaphore_signal(barrier, inc=1, device_id=(lax.rem(me + step, count),), device_id_type=MESH)
    pl.semaphore_wait(barrier, count - 1)

    def forward_copy(h, to_core, k):
        rows = pl.ds(h * half + k * CHUNK, CHUNK)
        return pltpu.make_async_remote_copy(
            src_ref=grads.at[diagonal * 2 + to_core, rows], dst_ref=rx.at[h, 0, core, pl.ds(k * CHUNK, CHUNK)],
            send_sem=p1_send.at[h, to_core, k], recv_sem=rx_sem.at[h, core, k],
            device_id=(first[h] * 2 + to_core,), device_id_type=MESH)

    def direct_copy(h, to_core, k):
        rows = pl.ds(h * half + k * DIRECT, DIRECT)
        return pltpu.make_async_remote_copy(
            src_ref=grads.at[first[h] * 2 + to_core, rows], dst_ref=rx.at[h, 1, core, pl.ds(k * DIRECT, DIRECT)],
            send_sem=direct_send.at[h, to_core, k], recv_sem=direct_sem.at[h, core, k],
            device_id=(first[h] * 2 + to_core,), device_id_type=MESH)

    def pair_copy(h, kind):
        owner = (second[h] if kind == 0 else chip) * 2 + 1 - core
        return pltpu.make_async_remote_copy(
            src_ref=grads.at[owner, pl.ds(h * half, half)], dst_ref=pd.at[h, kind],
            send_sem=pair_send.at[h, kind], recv_sem=pair_sem.at[h, kind],
            device_id=(partner,), device_id_type=MESH)

    def second_copy(h, k):
        rows = pl.ds(k * CHUNK, CHUNK)
        return pltpu.make_async_remote_copy(
            src_ref=stage.at[h, rows], dst_ref=inbox.at[h, rows],
            send_sem=p2_send.at[h, k], recv_sem=p2_sem.at[h, k],
            device_id=(second[h] * 2 + core,), device_id_type=MESH)

    for k in range(chunks):
        for h in range(2):
            for to_core in range(2):
                forward_copy(h, to_core, k).start()
        if k == 0:
            for h in range(2):
                pair_copy(h, 0).start()
        if k == 2:
            for h in range(2):
                pair_copy(h, 1).start()
    for k in range(directs):
        for h in range(2):
            for to_core in range(2):
                direct_copy(h, to_core, k).start()

    def loads(h, kind, k):
        owner = (second[h] if kind == 0 else chip) * 2 + core
        rows = pl.ds(k * CHUNK, CHUNK)
        copies = [
            pltpu.make_async_copy(grads.at[owner, pl.ds(h * half + k * CHUNK, CHUNK)], own, load_sem.at[0]),
            pltpu.make_async_copy(pd.at[h, kind, rows], other, load_sem.at[1]),
            pltpu.make_async_copy(rx.at[h, kind, 0, rows], near0, load_sem.at[2]),
            pltpu.make_async_copy(rx.at[h, kind, 1, rows], near1, load_sem.at[3]),
        ]
        for copy in copies:
            copy.start()
        for copy in copies:
            copy.wait()

    def four(rows):
        return (own[rows].astype(jnp.float32) + other[rows].astype(jnp.float32)) + (near0[rows].astype(jnp.float32) + near1[rows].astype(jnp.float32))

    for h in range(2):
        pair_copy(h, 0).wait_recv()

    def forward_step(k, carry):
        for h in range(2):
            for from_core in range(2):
                pltpu.make_async_copy(rx.at[h, 0, from_core, pl.ds(0, CHUNK)], rx.at[h, 0, from_core, pl.ds(0, CHUNK)], rx_sem.at[h, from_core, k]).wait()
            loads(h, 0, k)

            def add(group, carry):
                rows = pl.ds(pl.multiple_of(group * GROUP, GROUP), GROUP)
                tile[rows] = four(rows)
                return carry

            lax.fori_loop(0, CHUNK // GROUP, add, 0)
            put = pltpu.make_async_copy(tile, stage.at[h, pl.ds(k * CHUNK, CHUNK)], stage_sem.at[0])
            put.start()
            put.wait()
            second_copy(h, k).start()
        return carry

    lax.fori_loop(0, chunks, forward_step, 0)

    for h in range(2):
        pair_copy(h, 1).wait_recv()

    def own_step(k, carry):
        for h in range(2):
            loads(h, 1, k)

            def add(group, carry):
                base = pl.multiple_of(group * GROUP, GROUP)
                mine[pl.ds(pl.multiple_of(h * half + k * CHUNK + base, GROUP), GROUP)] = four(pl.ds(base, GROUP))
                return carry

            lax.fori_loop(0, CHUNK // GROUP, add, 0)
        return carry

    for part in range(directs):
        for h in range(2):
            for from_core in range(2):
                rows = pl.ds(part * DIRECT, DIRECT)
                pltpu.make_async_copy(rx.at[h, 1, from_core, rows], rx.at[h, 1, from_core, rows], direct_sem.at[h, from_core, part]).wait()
        lax.fori_loop(part * DIRECT // CHUNK, (part + 1) * DIRECT // CHUNK, own_step, 0)

    early = gathered.shape[1]
    span_rows = early // 2
    steps = span_rows // CHUNK
    late_steps = late.shape[0] // (2 * CHUNK)

    def early_row(h, k):
        return h * span_rows + k * CHUNK

    def late_row(h, k):
        return early + (2 * k + h) * CHUNK

    def state_copies(row, slot):
        return [pltpu.make_async_copy(source.at[pl.ds(row, CHUNK)], state.at[slot, i], state_sem.at[slot, i])
                for i, source in enumerate((master, mom_first, mom_second))]

    for h in range(2):
        for copy in state_copies(early_row(h, 0), h):
            copy.start()

    squares[...] = jnp.zeros_like(squares)

    def store(h, k):
        rows = pl.ds(h * half + k * CHUNK, CHUNK)
        return pltpu.make_async_copy(mine.at[rows], total.at[rows], store_sem.at[h, k])

    def owner_step(k, carry):
        for h in range(2):
            second_copy(h, k).wait_recv()

            def add(group, carry):
                base = pl.multiple_of(k * CHUNK + group * GROUP, GROUP)
                rows = pl.ds(pl.multiple_of(h * half + base, GROUP), GROUP)
                mean = (mine[rows] + inbox[h, pl.ds(base, GROUP)]) * (1.0 / count)
                mine[rows] = mean
                squares[...] += mean * mean
                return carry

            lax.fori_loop(0, CHUNK // GROUP, add, 0)
            store(h, k).start()
        return carry

    lax.fori_loop(0, chunks, owner_step, 0)

    lanes = jnp.sum(squares[...].reshape(GROUP // 8, 8, squares.shape[1]), axis=0)
    partial = lanes[:, 0:128]
    for column in range(1, squares.shape[1] // 128):
        partial += lanes[:, column * 128:(column + 1) * 128]
    norms[me] = partial

    def norm_copy(step):
        to = lax.rem(me + step, count)
        return pltpu.make_async_remote_copy(
            src_ref=norms.at[me], dst_ref=norms.at[me], send_sem=norm_send.at[step], recv_sem=norm_sem.at[me],
            device_id=(to,), device_id_type=MESH)

    for step in range(1, count):
        norm_copy(step).start()
    for step in range(1, count):
        source = lax.rem(me + step, count)
        pltpu.make_async_copy(norms.at[source], norms.at[source], norm_sem.at[source]).wait()
    square_sum = jnp.sum(jnp.sum(norms[...], axis=0))
    norm = jnp.sqrt(jnp.full(clip.shape, square_sum, jnp.float32))
    clip[...] = jnp.minimum(1.0, 1.0 / (norm + 1e-6))

    shard_rows = 2 * half
    near = (x_near * 2 + core, y_near * 2 + core)
    far = diagonal * 2 + core

    def span(h, k):
        return pl.ds(early_row(h, k), CHUNK)

    def near_copy(axis, h, k):
        return pltpu.make_async_remote_copy(
            src_ref=work.at[span(h, k)], dst_ref=gathered.at[me, span(h, k)],
            send_sem=near_send.at[axis, h, k], recv_sem=near_sem.at[axis, h, k],
            device_id=(near[axis],), device_id_type=MESH)

    def far_copy(h, k):
        return pltpu.make_async_remote_copy(
            src_ref=gathered.at[near[h], span(h, k)], dst_ref=gathered.at[near[h], span(h, k)],
            send_sem=far_send.at[h, k], recv_sem=far_sem.at[h, k],
            device_id=(near[1 - h],), device_id_type=MESH)

    def twin_copy(kind, h, k):
        if kind == 0:
            src, slab = work.at[span(h, k)], me
        else:
            slab = (near[0], near[1], far)[kind - 1]
            src = gathered.at[slab, span(h, k)]
        return pltpu.make_async_remote_copy(
            src_ref=src, dst_ref=gathered.at[slab, span(h, k)],
            send_sem=twin_send.at[kind, h, k], recv_sem=twin_sem.at[kind, h, k],
            device_id=(partner,), device_id_type=MESH)

    def arrived(slab, h, k, sem):
        pltpu.make_async_copy(gathered.at[slab, span(h, k)], gathered.at[slab, span(h, k)], sem).wait()

    def compute(row, slot, next_row):
        for copy in state_copies(row, slot):
            copy.wait()

        def update(group, carry):
            base = pl.multiple_of(group * TILE, TILE)
            here = pl.ds(base, TILE)
            there = pl.ds(pl.multiple_of(row + base, TILE), TILE)
            factor, decay = row_rules(me * shard_rows + row + base, TILE, runs)
            step_size = learn_rate[0] * factor
            for column in range(work.shape[1] // 128):
                lane = pl.ds(column * 128, 128)
                value = adam(mine[there, lane], clip[0:1, :], state[slot, 0, here, lane], state[slot, 1, here, lane], state[slot, 2, here, lane], step_size, decay)[0]
                work[there, lane] = value.astype(jnp.bfloat16)
            return carry

        lax.fori_loop(0, CHUNK // TILE, update, 0)
        if next_row is not None:
            for copy in state_copies(next_row, slot):
                copy.start()

    def early_step(k, carry):
        for h in range(2):
            compute(early_row(h, k), h, early_row(h, k + 1))
            near_copy(h, h, k).start()
            twin_copy(0, h, k).start()
        return carry

    lax.fori_loop(0, steps - 1, early_step, 0)
    for h in range(2):
        compute(early_row(h, steps - 1), h, late_row(h, 0))
        near_copy(h, h, steps - 1).start()
        twin_copy(0, h, steps - 1).start()

    def other_step(k, carry):
        for h in range(2):
            near_copy(1 - h, h, k).start()
        return carry

    lax.fori_loop(0, steps, other_step, 0)
    keep = pltpu.make_async_copy(work.at[pl.ds(0, early)], gathered.at[me], copy_sem.at[0])
    keep.start()

    def late_step(k, carry):
        for h in range(2):
            compute(late_row(h, k), h, late_row(h, k + 1))
        return carry

    lax.fori_loop(0, late_steps - 1, late_step, 0)
    for h in range(2):
        compute(late_row(h, late_steps - 1), h, None)
    leave = pltpu.make_async_copy(work.at[pl.ds(early, late.shape[0])], late, copy_sem.at[1])
    leave.start()

    def first_step(k, carry):
        for h in range(2):
            arrived(near[h], h, k, near_sem.at[h, h, k])
            far_copy(h, k).start()
            twin_copy(1 + h, h, k).start()
        return carry

    lax.fori_loop(0, steps, first_step, 0)

    def second_step(k, carry):
        for axis in range(2):
            arrived(near[axis], 1 - axis, k, near_sem.at[axis, 1 - axis, k])
            twin_copy(1 + axis, 1 - axis, k).start()
        return carry

    lax.fori_loop(0, steps, second_step, 0)

    def finish_reduce(k, carry):
        for h in range(2):
            for to_core in range(2):
                forward_copy(h, to_core, k).wait_send()
            second_copy(h, k).wait_send()
            store(h, k).wait()
        return carry

    lax.fori_loop(0, chunks, finish_reduce, 0)
    for h in range(2):
        for to_core in range(2):
            for k in range(directs):
                direct_copy(h, to_core, k).wait_send()
        for kind in range(2):
            pair_copy(h, kind).wait_send()
    for step in range(1, count):
        norm_copy(step).wait_send()
    keep.wait()
    leave.wait()

    def third_step(k, carry):
        for h in range(2):
            arrived(far, h, k, far_sem.at[h, k])
            twin_copy(3, h, k).start()
        return carry

    lax.fori_loop(0, steps, third_step, 0)

    def finish(k, carry):
        twin = (partner, x_near * 2 + 1 - core, y_near * 2 + 1 - core, diagonal * 2 + 1 - core)
        for h in range(2):
            for axis in range(2):
                near_copy(axis, h, k).wait_send()
            far_copy(h, k).wait_send()
            for kind in range(4):
                twin_copy(kind, h, k).wait_send()
                arrived(twin[kind], h, k, twin_sem.at[kind, h, k])
        return carry

    lax.fori_loop(0, steps, finish, 0)


def reduce_and_gather(local_grads, master, mom_first, mom_second, rate, runs, count):
    _, total_rows, width = local_grads.shape
    rows = total_rows // count
    half = rows // 2
    early = rows - LATE
    chunks, directs, steps = half // CHUNK, half // DIRECT, early // 2 // CHUNK
    any_space = pl.BlockSpec(memory_space=pl.ANY)
    dma = pltpu.SemaphoreType.DMA
    outs = pl.pallas_call(
        functools.partial(step_kernel, half, runs),
        name="reduce_and_gather",
        out_shape=(
            jax.ShapeDtypeStruct((rows, width), jnp.float32),
            jax.ShapeDtypeStruct((8, 128), jnp.float32),
            jax.ShapeDtypeStruct((2, 2, 2, half, width), jnp.bfloat16),
            jax.ShapeDtypeStruct((2, 2, half, width), jnp.bfloat16),
            jax.ShapeDtypeStruct((2, half, width), jnp.float32),
            jax.ShapeDtypeStruct((count, early, width), jnp.bfloat16),
            jax.ShapeDtypeStruct((LATE, width), jnp.bfloat16),
        ),
        in_specs=[pl.BlockSpec(memory_space=pltpu.SMEM)] + [any_space] * 4,
        out_specs=(any_space, pl.BlockSpec(memory_space=pltpu.VMEM)) + (any_space,) * 5,
        scratch_shapes=[
            pltpu.VMEM((2, half, width), jnp.float32),
            pltpu.VMEM((rows, width), jnp.float32),
            pltpu.VMEM((CHUNK, width), jnp.bfloat16),
            pltpu.VMEM((CHUNK, width), jnp.bfloat16),
            pltpu.VMEM((CHUNK, width), jnp.bfloat16),
            pltpu.VMEM((CHUNK, width), jnp.bfloat16),
            pltpu.VMEM((CHUNK, width), jnp.float32),
            pltpu.VMEM((GROUP, width), jnp.float32),
            pltpu.VMEM((count, 8, 128), jnp.float32),
            pltpu.VMEM((2, 3, CHUNK, width), jnp.float32),
            pltpu.VMEM((rows, width), jnp.bfloat16),
            dma((2, 2, chunks)), dma((2, 2, directs)), dma((2, 2)), dma((2, chunks)), dma((count,)),
            dma((2, 2, chunks)), dma((2, 2, directs)), dma((2, 2)), dma((2, chunks)), dma((count,)),
            dma((4,)), dma((2, chunks)), dma((1,)), dma((2, 3)), dma((2,)),
            dma((2, 2, steps)), dma((2, steps)), dma((4, 2, steps)), dma((2, 2, steps)), dma((2, steps)), dma((4, 2, steps)),
        ],
        compiler_params=pltpu.CompilerParams(collective_id=0, has_side_effects=True, vmem_limit_bytes=62 * 1024 * 1024),
    )(rate, local_grads.reshape(count, rows, width), master, mom_first, mom_second)
    return outs[0], outs[1], outs[5], outs[6]


def update_kernel(shard_rows, runs, learn_rate, clip, grad, master, first, second, new_master, new_first, new_second, working):
    block = grad.shape[0]
    factor, decay = row_rules(lax.axis_index("dp") * shard_rows + pl.program_id(0) * block, block, runs)
    step_size = learn_rate[0] * factor
    for column in range(grad.shape[1] // 128):
        lanes = pl.ds(column * 128, 128)
        value, first_value, second_value = adam(grad[:, lanes], clip[0:1, :], master[:, lanes], first[:, lanes], second[:, lanes], step_size, decay)
        new_master[:, lanes] = value
        new_first[:, lanes] = first_value
        new_second[:, lanes] = second_value


def update_rows(runs, count, learn_rate, clip, grad, master, first, second):
    shard_rows, width = grad.shape
    block = pl.BlockSpec((BLOCK, width), lambda i: (i, 0))
    whole = jax.ShapeDtypeStruct((shard_rows, width), jnp.float32)
    size = shard_rows * width
    return pl.pallas_call(
        functools.partial(update_kernel, shard_rows, runs),
        name="update_rows",
        grid=(shard_rows // BLOCK,),
        out_shape=(whole, whole, whole, jax.ShapeDtypeStruct((shard_rows * count, width), jnp.bfloat16)),
        in_specs=[pl.BlockSpec(memory_space=pltpu.SMEM), pl.BlockSpec((8, 128), lambda i: (0, 0)), block, block, block, block],
        out_specs=(block, block, block, pl.BlockSpec(memory_space=pl.ANY)),
        cost_estimate=pl.CostEstimate(flops=20 * size, bytes_accessed=28 * size, transcendentals=2 * size),
        compiler_params=pltpu.CompilerParams(dimension_semantics=("arbitrary",), vmem_limit_bytes=48 * 1024 * 1024),
    )(learn_rate, clip, grad, master, first, second)


def place_kernel(start, gathered, working_in, working, ring, in_sem, out_sem):
    count, rows, _ = gathered.shape
    shard_rows = working.shape[0] // count
    pieces = [(device, row) for row in range(0, rows, PIECE) for device in range(count)]

    def read(i):
        device, row = pieces[i]
        return pltpu.make_async_copy(gathered.at[device, pl.ds(row, PIECE)], ring.at[i % DEPTH], in_sem.at[i % DEPTH])

    def write(i):
        device, row = pieces[i]
        return pltpu.make_async_copy(ring.at[i % DEPTH], working.at[pl.ds(device * shard_rows + start + row, PIECE)], out_sem.at[i % DEPTH])

    lead = DEPTH // 2
    for i in range(len(pieces) + lead):
        if i < len(pieces):
            if i >= DEPTH:
                write(i - DEPTH).wait()
            read(i).start()
        if i >= lead:
            read(i - lead).wait()
            write(i - lead).start()
    for i in range(max(0, len(pieces) - DEPTH), len(pieces)):
        write(i).wait()


def place_rows(start, working, gathered):
    count, rows, width = gathered.shape
    size = rows * width * count
    any_space = pl.BlockSpec(memory_space=pl.ANY)
    return pl.pallas_call(
        functools.partial(place_kernel, start),
        name="place_rows",
        out_shape=jax.ShapeDtypeStruct(working.shape, working.dtype),
        in_specs=[any_space, any_space],
        out_specs=any_space,
        input_output_aliases={1: 0},
        scratch_shapes=[
            pltpu.VMEM((DEPTH, PIECE, width), working.dtype),
            pltpu.SemaphoreType.DMA((DEPTH,)),
            pltpu.SemaphoreType.DMA((DEPTH,)),
        ],
        cost_estimate=pl.CostEstimate(flops=size, bytes_accessed=4 * size, transcendentals=0),
        compiler_params=pltpu.CompilerParams(vmem_limit_bytes=48 * 1024 * 1024),
    )(gathered, working)


def solution(mesh):
    count = mesh.shape["dp"]

    def device_step(local_grads, master, mom_first, mom_second, learn_rate):
        shard_rows, width = master.shape
        total_rows = shard_rows * count
        runs = layout_runs(width, total_rows)
        rate = learn_rate.reshape(1)
        grad, clip, early, block = reduce_and_gather(local_grads, master, mom_first, mom_second, rate, runs, count)
        late = lax.all_gather(block, "dp", axis=0, tiled=False)
        new_master, new_first, new_second, working = update_rows(runs, count, rate, clip, grad, master, mom_first, mom_second)
        working = place_rows(0, working, early)
        working = place_rows(shard_rows - LATE, working, late)
        return new_master, new_first, new_second, working

    return jax.shard_map(device_step, mesh=mesh, in_specs=(P("dp", None, None), P("dp", None), P("dp", None), P("dp", None), P()), out_specs=(P("dp", None), P("dp", None), P("dp", None), P(None, None)), check_vma=False)
```
